32 devices in a mesh: row: 16 (over z, y, x), col: 2 (over core).
Axes of the slice: x: 2, y: 2, z: 4, core: 2. Of those that a mesh axis runs over, the one named last changes fastest.
Arguments:
- messages: float32 [32, 16, 2, 16, 128], P(('row', 'col')), may hold values from -6 to 6
- dst_local: int32 [32, 16, 2, 16], P(('row', 'col')), may hold values from 0 to 255
- counts: int32 [32, 16, 2], P(('row', 'col')), may hold values from 8 to 16, as said below
- degrees: int32 [8192], P(('row', 'col')), may hold values from 1 to 8
Outputs:
- aggregate: float32 [8192, 128], P(('row', 'col'))
The draws below stay inside these ranges and needn't reach their ends.
Inputs may be any that keep to these rules, and one draw needn't show every extreme that they name: For every sender and group, the counts over the group's 2 ranges sum to exactly 24. In each group one range receives 16 live slots from every sender.
All inputs are finite; a program needn't handle non-finite values.
Results may differ from the reference program's by a relative error of at most 0.0003.
Values sent between devices are 32-bit elements; how exact they have to be, the bound alone decides.
No kernel may reach another device: no remote copies, remote signals or barrier semaphores. Data moves between devices by JAX's collectives and lax.ppermute only.
A program may use at most 64 MiB of HBM per device.

```python
import math
import jax
import jax.numpy as jnp
import numpy as np
from jax import lax

W = 128
V_DEV = 256
CAPC = 16
GROUPS = 16
SUBS = 2
SENDERS = 32
VERTICES = 8192


def draw_counts(key, part):
    first, second = jax.random.split(jax.random.fold_in(key, 11), 2)
    half = CAPC // 2
    dropped = SUBS * half // 2
    tokens = max((SUBS - 1) * half, 1)
    hot = jax.random.randint(first, (GROUPS,), 0, SUBS)
    keys = jax.random.split(second, SENDERS * GROUPS)
    perms = jax.vmap(lambda k: jax.random.permutation(k, tokens))(keys)
    chosen = (perms < dropped).astype(jnp.int32)
    owner = jnp.arange(tokens) // max(half, 1)
    onehot = (owner[:, None] == jnp.arange(SUBS - 1)[None, :]).astype(jnp.int32)
    loss_other = jnp.dot(chosen, onehot).reshape(SENDERS, GROUPS, SUBS - 1)
    ranges = jnp.arange(SUBS)
    hot_b = hot[None, :, None]
    other_index = jnp.where(ranges[None, None, :] < hot_b, ranges[None, None, :], ranges[None, None, :] - 1)
    other_index = jnp.clip(other_index, 0, SUBS - 2)
    picked = jnp.take_along_axis(loss_other, jnp.broadcast_to(other_index, (SENDERS, GROUPS, SUBS)), axis=2)
    loss = jnp.where(ranges[None, None, :] == hot_b, 0, picked)
    return (CAPC - loss).astype(jnp.int32)


def set_ends(entries, own_key, low, high):
    dims = entries.shape
    place = [jax.random.randint(jax.random.fold_in(own_key, axis), (), 0, dims[axis]) for axis in range(len(dims))]
    entries = entries.at[tuple(place)].set(low)
    longest = dims.index(max(dims))
    place[longest] = (place[longest] + 1) % dims[longest]
    return entries.at[tuple(place)].set(high)


def levels(key, shape, shards, least, high):
    def one(axis_at, blocks):
        steps = jax.random.uniform(jax.random.fold_in(jax.random.fold_in(key, 6), axis_at), (blocks,), jnp.float32, least / len(shards), high / len(shards))
        return jnp.repeat(jnp.exp(steps), shape[axis_at] // blocks).reshape((-1,) + (1,) * (len(shape) - axis_at - 1))

    level = one(*shards[0])
    for cut in shards[1:]:
        level = level * one(*cut)
    return level


def cumulative_ranks(amount, lean):
    portions = [(1 << 20) // math.isqrt(grade ** lean) + 1 for grade in range(1, amount + 1)]
    width = 1 + sum(portions) // (1 << 30)
    return np.cumsum(np.array([max(1, weight // width) for weight in portions]))


def ranked(key, extent, count, slope):
    listing = cumulative_ranks(count, slope)
    lot = jax.random.randint(jax.random.fold_in(key, 1), extent, 0, int(listing[count - 1]))
    grade = jnp.searchsorted(jnp.asarray(listing, jnp.int32), lot, side="right")
    return jax.random.permutation(jax.random.fold_in(key, 2), count)[grade].astype(jnp.int32)


def centred(stream_key, shape, spread, limit, shards=(), held_as=jnp.bfloat16):
    array = jax.random.normal(stream_key, shape, jnp.float32) * spread
    if len(shards) > 0:
        array = levels(stream_key, shape, shards, -0.22, 0.18) * array
    return jnp.clip(array, min=-limit, max=limit).astype(held_as)


def setup_inputs(seed: int = 0) -> dict:
    streams_of = jax.random.split(jax.random.key(seed), 5)
    return {
        "messages": centred(streams_of[0], (SENDERS, GROUPS, SUBS, CAPC, W), 1.0, 6.0, ((0, 32),), jnp.float32),
        "dst_local": set_ends(ranked(streams_of[1], (SENDERS, GROUPS, SUBS, CAPC), V_DEV, 2), jax.random.fold_in(streams_of[1], 3), 0, V_DEV - 1).astype(jnp.int32),
        "counts": draw_counts(jax.random.fold_in(streams_of[4], 71), 0),
        "degrees": set_ends(jax.random.randint(streams_of[3], (VERTICES,), 1, 9), jax.random.fold_in(streams_of[3], 1), 1, 8).astype(jnp.int32),
    }


def reference(messages, dst_local, counts, degrees):
    slot_index = jnp.arange(CAPC).astype(jnp.int32)
    group_index = jnp.arange(GROUPS).astype(jnp.int32)[:, None, None]
    range_index = jnp.arange(SUBS).astype(jnp.int32)[None, :, None]

    def accumulate(running, element):
        block, targets_local, count_block = element
        alive_mask = (slot_index[None, None, :] < count_block[:, :, None]).astype(jnp.float32)
        target = ((group_index * SUBS + range_index) * V_DEV + targets_local).astype(jnp.int32)
        values = block * alive_mask[..., None]
        running = running.at[target.reshape(-1)].add(values.reshape(-1, W))
        return running, None

    start = jnp.zeros((VERTICES, W), jnp.float32)
    summed, _ = lax.scan(accumulate, start, (messages, dst_local, counts))
    scale = jnp.maximum(degrees, 1).astype(jnp.float32)
    return summed / scale[:, None]
```

```python
import jax
import jax.numpy as jnp
from jax import lax
from jax.experimental import pallas as pl
from jax.experimental.pallas import tpu as pltpu
from jax.sharding import PartitionSpec as P

LANES = 128
SUBLANES = 8


def general(messages, dst_local, counts, degrees):
    slots = messages.shape[3]
    width = messages.shape[4]
    owned = degrees.shape[0]
    slot_index = lax.broadcasted_iota(jnp.int32, counts.shape + (slots,), 3)
    alive_mask = (slot_index < counts[..., None]).astype(jnp.float32)
    masked = messages * alive_mask[..., None]

    def exchange(x):
        x = lax.all_to_all(x, "row", split_axis=1, concat_axis=0, tiled=True)
        return lax.all_to_all(x, "col", split_axis=2, concat_axis=1, tiled=True)

    received, labels = exchange(masked), exchange(dst_local)
    summed = jax.ops.segment_sum(received.reshape(-1, width), labels.reshape(-1), num_segments=owned)
    scale = jnp.maximum(degrees, 1).astype(jnp.float32)
    return summed / scale[:, None]


def meeting_order(rows):
    first = rows * 5 // 8
    return [first] + [r for r in range(1, rows) if r != first] + [0]


def pack_kernel(order, owned, counts_ref, dst_ref, messages_ref, out_ref):
    groups, _, slots, width = messages_ref.shape
    half = slots // 2
    live = slots + half
    pitch = live + 1
    lane = lax.broadcasted_iota(jnp.int32, (groups, width), 1)
    group = lax.broadcasted_iota(jnp.int32, (groups, width), 0)
    full = [counts_ref[0, g] == slots for g in range(groups)]
    full_rows = jnp.zeros((groups, width), jnp.int32)
    for g in range(groups):
        full_rows = jnp.where(group == g, full[g].astype(jnp.int32), full_rows)
    fill = jnp.zeros((groups, width - slots), jnp.int32)
    first = jnp.concatenate([dst_ref[pl.ds(0, groups, stride=2), :], fill], axis=1)
    second = jnp.concatenate([dst_ref[pl.ds(1, groups, stride=2), :], fill], axis=1) + owned
    by_half = pltpu.roll(second, half, 1)
    by_full = pltpu.roll(second, slots, 1)
    when_full = jnp.where(lane < slots, first, by_full)
    when_half = jnp.where(lane < half, first, by_half)
    labels = jnp.where(full_rows == 1, when_full, when_half).astype(jnp.float32)
    for place, g in enumerate(order):
        base = place * pitch
        a0 = messages_ref[g, 0, :half, :]
        a1 = messages_ref[g, 0, half:, :]
        b0 = messages_ref[g, 1, :half, :]
        b1 = messages_ref[g, 1, half:, :]
        out_ref[base : base + half, :] = a0
        out_ref[base + half : base + slots, :] = jnp.where(full[g], a1, b0)
        out_ref[base + slots : base + live, :] = jnp.where(full[g], b0, b1)
        out_ref[base + live : base + pitch, :] = labels[g : g + 1, :]


def sum_kernel(rows, owned, received_ref, own_ref, other_ref):
    width = received_ref.shape[1]
    pitch = received_ref.shape[0] // rows
    live = pitch - 1
    total = rows * live
    labels = received_ref[pl.ds(live, rows, stride=pitch), :].astype(jnp.int32)
    left = live
    while left:
        step = min(left, (width - 1) // (rows - 1))
        labels = pltpu.roll(labels, 0, 1, stride=step, stride_axis=0)
        left -= step
    place = lax.broadcasted_iota(jnp.int32, (rows, width), 0)
    lane = lax.broadcasted_iota(jnp.int32, (rows, width), 1)
    slot = lax.rem(lane - lax.rem(place * live, width) + width, width)
    position = place * live + slot
    parts = []
    for block in range(total // width):
        inside = (slot < live) & (position >= block * width) & (position < (block + 1) * width)
        parts.append(jnp.sum(jnp.where(inside, labels, 0), axis=0, keepdims=True))
    label = jnp.concatenate(parts, axis=1)
    values = jnp.concatenate([received_ref[p * pitch : p * pitch + live, :] for p in range(rows)], axis=0)
    high = values.astype(jnp.bfloat16)
    low = (values - high.astype(jnp.float32)).astype(jnp.bfloat16)
    both = jnp.concatenate([high, low], axis=1)
    vertex = lax.broadcasted_iota(jnp.int32, (owned, total), 0)
    core = lax.axis_index("col")
    for ref, side in ((other_ref, 1 - core), (own_ref, core)):
        hot = (vertex == label - side * owned).astype(jnp.float32).astype(jnp.bfloat16)
        sums = jnp.dot(hot, both, preferred_element_type=jnp.float32)
        ref[...] = sums[:, :width] + sums[:, width:]


def paired(rows, messages, dst_local, counts, degrees):
    _, groups, subs, slots, width = messages.shape
    owned = degrees.shape[0]
    pitch = slots + slots // 2 + 1
    order = meeting_order(rows)
    vmem = pl.BlockSpec(memory_space=pltpu.VMEM)
    packed = pl.pallas_call(
        lambda *refs: pack_kernel(order, owned, *refs),
        out_shape=jax.ShapeDtypeStruct((groups * pitch, width), jnp.float32),
        in_specs=[pl.BlockSpec(memory_space=pltpu.SMEM), vmem, vmem],
        out_specs=vmem,
        name="pack",
    )(counts.reshape(groups, subs).T, dst_local.reshape(groups * subs, slots), messages[0])
    received = lax.all_to_all(
        packed.reshape(groups * pitch, 1, width),
        "row",
        split_axis=0,
        concat_axis=0,
        tiled=True,
        axis_index_groups=[order],
    ).reshape(groups * pitch, width)
    own, other = pl.pallas_call(
        lambda *refs: sum_kernel(rows, owned, *refs),
        out_shape=[jax.ShapeDtypeStruct((owned, width), jnp.float32)] * 2,
        in_specs=[vmem],
        out_specs=[vmem, vmem],
        name="sum_slots",
    )(received)
    mine = lax.ppermute(other, "col", [(0, 1), (1, 0)])
    scale = jnp.maximum(degrees, 1).astype(jnp.float32)
    return (own + mine) / scale[:, None]


def solution(mesh):
    rows, cols = mesh.shape["row"], mesh.shape["col"]

    def body(messages, dst_local, counts, degrees):
        subs, slots, width = messages.shape[2:]
        live = slots + slots // 2
        fits = width == LANES and slots % (2 * SUBLANES) == 0 and rows * live % width == 0
        if subs == cols == 2 and fits and rows <= 16:
            return paired(rows, messages, dst_local, counts, degrees)
        return general(messages, dst_local, counts, degrees)

    in_specs = (
        P(("row", "col"), None, None, None, None),
        P(("row", "col"), None, None, None),
        P(("row", "col"), None, None),
        P(("row", "col")),
    )
    out_specs = P(("row", "col"), None)
    return jax.shard_map(body, mesh=mesh, in_specs=in_specs, out_specs=out_specs, check_vma=False)
```

```python
import jax
import jax.numpy as jnp
from jax import lax
from jax.experimental import pallas as pl
from jax.experimental.pallas import tpu as pltpu
from jax.sharding import PartitionSpec as P

LANES = 128
SUBLANES = 8
SMALL = pltpu.CompilerParams(vmem_limit_bytes=8 << 20)


def general(messages, dst_local, counts, degrees):
    slots = messages.shape[3]
    width = messages.shape[4]
    owned = degrees.shape[0]
    slot_index = lax.broadcasted_iota(jnp.int32, counts.shape + (slots,), 3)
    alive_mask = (slot_index < counts[..., None]).astype(jnp.float32)
    masked = messages * alive_mask[..., None]

    def exchange(x):
        x = lax.all_to_all(x, "row", split_axis=1, concat_axis=0, tiled=True)
        return lax.all_to_all(x, "col", split_axis=2, concat_axis=1, tiled=True)

    received, labels = exchange(masked), exchange(dst_local)
    summed = jax.ops.segment_sum(received.reshape(-1, width), labels.reshape(-1), num_segments=owned)
    scale = jnp.maximum(degrees, 1).astype(jnp.float32)
    return summed / scale[:, None]


def in_hbm(x):
    return pltpu.with_memory_space_constraint(x, pltpu.HBM)


def meeting_order(rows):
    first = rows * 5 // 8
    return [first] + [r for r in range(1, rows) if r != first] + [0]


def pack_kernel(order, owned, counts_hbm, dst_hbm, messages_hbm, out_ref, counts_ref, dst_ref, messages_ref, sems):
    fetches = [
        pltpu.make_async_copy(source, target, sems.at[i])
        for i, (source, target) in enumerate(
            ((counts_hbm, counts_ref), (dst_hbm, dst_ref), (messages_hbm, messages_ref))
        )
    ]
    for fetch in fetches:
        fetch.start()
    groups, _, slots, width = messages_ref.shape
    half = slots // 2
    live = slots + half
    pitch = live + 1
    for fetch in fetches[:2]:
        fetch.wait()
    lane = lax.broadcasted_iota(jnp.int32, (groups, width), 1)
    group = lax.broadcasted_iota(jnp.int32, (groups, width), 0)
    full = [counts_ref[0, g] == slots for g in range(groups)]
    full_rows = jnp.zeros((groups, width), jnp.int32)
    for g in range(groups):
        full_rows = jnp.where(group == g, full[g].astype(jnp.int32), full_rows)
    fill = jnp.zeros((groups, width - slots), jnp.int32)
    first = jnp.concatenate([dst_ref[pl.ds(0, groups, stride=2), :], fill], axis=1)
    second = jnp.concatenate([dst_ref[pl.ds(1, groups, stride=2), :], fill], axis=1) + owned
    by_half = pltpu.roll(second, half, 1)
    by_full = pltpu.roll(second, slots, 1)
    when_full = jnp.where(lane < slots, first, by_full)
    when_half = jnp.where(lane < half, first, by_half)
    labels = jnp.where(full_rows == 1, when_full, when_half).astype(jnp.float32)
    fetches[2].wait()
    for place, g in enumerate(order):
        base = place * pitch
        a0 = messages_ref[g, 0, :half, :]
        a1 = messages_ref[g, 0, half:, :]
        b0 = messages_ref[g, 1, :half, :]
        b1 = messages_ref[g, 1, half:, :]
        out_ref[base : base + half, :] = a0
        out_ref[base + half : base + slots, :] = jnp.where(full[g], a1, b0)
        out_ref[base + slots : base + live, :] = jnp.where(full[g], b0, b1)
        out_ref[base + live : base + pitch, :] = labels[g : g + 1, :]


def slot_values(rows, received_ref, both_ref, label_ref):
    width = received_ref.shape[1]
    pitch = received_ref.shape[0] // rows
    live = pitch - 1
    total = rows * live
    labels = received_ref[pl.ds(live, rows, stride=pitch), :].astype(jnp.int32)
    left = live
    while left:
        step = min(left, (width - 1) // (rows - 1))
        labels = pltpu.roll(labels, 0, 1, stride=step, stride_axis=0)
        left -= step
    place = lax.broadcasted_iota(jnp.int32, (rows, width), 0)
    lane = lax.broadcasted_iota(jnp.int32, (rows, width), 1)
    slot = lax.rem(lane - lax.rem(place * live, width) + width, width)
    position = place * live + slot
    parts = []
    for block in range(total // width):
        inside = (slot < live) & (position >= block * width) & (position < (block + 1) * width)
        parts.append(jnp.sum(jnp.where(inside, labels, 0), axis=0, keepdims=True))
    label = jnp.concatenate(parts, axis=1)
    values = jnp.concatenate([received_ref[p * pitch : p * pitch + live, :] for p in range(rows)], axis=0)
    high = values.astype(jnp.bfloat16)
    low = (values - high.astype(jnp.float32)).astype(jnp.bfloat16)
    both = jnp.concatenate([high, low], axis=1)
    both_ref[...] = both
    label_ref[...] = jnp.broadcast_to(label, label_ref.shape)
    return both, label


def range_sums(owned, side, both, label):
    width = both.shape[1] // 2
    vertex = lax.broadcasted_iota(jnp.int32, (owned, both.shape[0]), 0)
    hot = (vertex == label - side * owned).astype(jnp.float32).astype(jnp.bfloat16)
    sums = jnp.dot(hot, both, preferred_element_type=jnp.float32)
    return sums[:, :width] + sums[:, width:]


def other_kernel(rows, owned, received_ref, other_ref, both_ref, label_ref):
    both, label = slot_values(rows, received_ref, both_ref, label_ref)
    other_ref[...] = range_sums(owned, 1 - lax.axis_index("col"), both, label)


def own_kernel(owned, both_ref, label_ref, degrees_ref, own_ref, share_ref):
    width = own_ref.shape[1]
    sums = range_sums(owned, lax.axis_index("col"), both_ref[...], label_ref[0:1, :])
    for start in range(0, owned, width):
        scale = jnp.maximum(degrees_ref[0:1, start : start + width], 1).astype(jnp.float32)
        share = jnp.transpose(jnp.broadcast_to(1.0 / scale, (width, width)))
        share_ref[start : start + width, :] = share
        own_ref[start : start + width, :] = sums[start : start + width, :] * share


def last_kernel(pieces, own_ref, mine_ref, share_ref, out_hbm, out_ref, sems):
    size = out_ref.shape[0] // pieces
    copies = []
    for i in range(pieces):
        piece = slice(i * size, (i + 1) * size)
        out_ref[piece, :] = own_ref[piece, :] + mine_ref[piece, :] * share_ref[piece, :]
        copies.append(pltpu.make_async_copy(out_ref.at[piece, :], out_hbm.at[piece, :], sems.at[i]))
        copies[-1].start()
    for copy in copies:
        copy.wait()


def paired(rows, messages, dst_local, counts, degrees):
    _, groups, subs, slots, width = messages.shape
    owned = degrees.shape[0]
    pitch = slots + slots // 2 + 1
    order = meeting_order(rows)
    total = rows * (pitch - 1)
    vmem = pl.BlockSpec(memory_space=pltpu.VMEM)
    hbm = pl.BlockSpec(memory_space=pltpu.HBM)
    packed = pl.pallas_call(
        lambda *refs: pack_kernel(order, owned, *refs),
        out_shape=jax.ShapeDtypeStruct((groups * pitch, width), jnp.float32),
        in_specs=[hbm, hbm, hbm],
        out_specs=vmem,
        scratch_shapes=[
            pltpu.SMEM((subs, groups), jnp.int32),
            pltpu.VMEM((groups * subs, slots), jnp.int32),
            pltpu.VMEM((groups, subs, slots, width), jnp.float32),
            pltpu.SemaphoreType.DMA((3,)),
        ],
        compiler_params=SMALL,
        name="pack",
    )(in_hbm(counts.reshape(groups, subs).T), in_hbm(dst_local.reshape(groups * subs, slots)), in_hbm(messages[0]))
    received = lax.all_to_all(
        packed.reshape(groups * pitch, 1, width),
        "row",
        split_axis=0,
        concat_axis=0,
        tiled=True,
        axis_index_groups=[order],
    ).reshape(groups * pitch, width)
    partial = jax.ShapeDtypeStruct((owned, width), jnp.float32)
    other, both, label = pl.pallas_call(
        lambda *refs: other_kernel(rows, owned, *refs),
        out_shape=[
            partial,
            jax.ShapeDtypeStruct((total, 2 * width), jnp.bfloat16),
            jax.ShapeDtypeStruct((SUBLANES, total), jnp.int32),
        ],
        in_specs=[vmem],
        out_specs=[vmem] * 3,
        compiler_params=SMALL,
        name="other_sums",
    )(received)
    mine = lax.ppermute(other, "col", [(0, 1), (1, 0)])
    own, share = pl.pallas_call(
        lambda *refs: own_kernel(owned, *refs),
        out_shape=[partial, partial],
        in_specs=[vmem] * 3,
        out_specs=[vmem] * 2,
        compiler_params=SMALL,
        cost_estimate=pl.CostEstimate(flops=4 * owned * total * width, bytes_accessed=1 << 20, transcendentals=0),
        name="own_sums",
    )(both, label, degrees.reshape(1, owned))
    pieces = 4
    return pl.pallas_call(
        lambda *refs: last_kernel(pieces, *refs),
        out_shape=partial,
        in_specs=[vmem] * 3,
        out_specs=hbm,
        scratch_shapes=[pltpu.VMEM((owned, width), jnp.float32), pltpu.SemaphoreType.DMA((pieces,))],
        compiler_params=SMALL,
        name="mean",
    )(own, mine, share)


def solution(mesh):
    rows, cols = mesh.shape["row"], mesh.shape["col"]

    def body(messages, dst_local, counts, degrees):
        subs, slots, width = messages.shape[2:]
        live = slots + slots // 2
        fits = width == LANES and slots % (2 * SUBLANES) == 0 and rows * live % width == 0
        if subs == cols == 2 and fits and rows <= 16:
            return paired(rows, messages, dst_local, counts, degrees)
        return general(messages, dst_local, counts, degrees)

    in_specs = (
        P(("row", "col"), None, None, None, None),
        P(("row", "col"), None, None, None),
        P(("row", "col"), None, None),
        P(("row", "col")),
    )
    out_specs = P(("row", "col"), None)
    return jax.shard_map(body, mesh=mesh, in_specs=in_specs, out_specs=out_specs, check_vma=False)
```

```python
import jax
import jax.numpy as jnp
from jax import lax
from jax.experimental import pallas as pl
from jax.experimental.pallas import tpu as pltpu
from jax.sharding import PartitionSpec as P

LANES = 128
SUBLANES = 8
SMALL = pltpu.CompilerParams(vmem_limit_bytes=8 << 20)


def general(messages, dst_local, counts, degrees):
    slots = messages.shape[3]
    width = messages.shape[4]
    owned = degrees.shape[0]
    slot_index = lax.broadcasted_iota(jnp.int32, counts.shape + (slots,), 3)
    alive_mask = (slot_index < counts[..., None]).astype(jnp.float32)
    masked = messages * alive_mask[..., None]

    def exchange(x):
        x = lax.all_to_all(x, "row", split_axis=1, concat_axis=0, tiled=True)
        return lax.all_to_all(x, "col", split_axis=2, concat_axis=1, tiled=True)

    received, labels = exchange(masked), exchange(dst_local)
    summed = jax.ops.segment_sum(received.reshape(-1, width), labels.reshape(-1), num_segments=owned)
    scale = jnp.maximum(degrees, 1).astype(jnp.float32)
    return summed / scale[:, None]


def in_hbm(x):
    return pltpu.with_memory_space_constraint(x, pltpu.HBM)


ORDERS = {16: (11, 8, 5, 3, 13, 14, 4, 2, 15, 12, 7, 9, 10, 1, 6, 0)}


def meeting_order(rows):
    first = rows * 3 // 4 - 1
    return ORDERS.get(rows, (first, *(r for r in range(1, rows) if r != first), 0))


def exchange_groups(order, cols):
    swap = [int(2 * r >= len(order)) for r in order]
    return [[r * cols + (c ^ s) for r, s in zip(order, swap)] for c in range(cols)]


def pack_kernel(order, owned, counts_hbm, dst_hbm, messages_hbm, out_ref, counts_ref, dst_ref, messages_ref, sems):
    fetches = [
        pltpu.make_async_copy(source, target, sems.at[i])
        for i, (source, target) in enumerate(
            ((counts_hbm, counts_ref), (dst_hbm, dst_ref), (messages_hbm, messages_ref))
        )
    ]
    for fetch in fetches:
        fetch.start()
    groups, _, slots, width = messages_ref.shape
    half = slots // 2
    live = slots + half
    pitch = live + 1
    for fetch in fetches[:2]:
        fetch.wait()
    lane = lax.broadcasted_iota(jnp.int32, (groups, width), 1)
    group = lax.broadcasted_iota(jnp.int32, (groups, width), 0)
    full = [counts_ref[0, g] == slots for g in range(groups)]
    full_rows = jnp.zeros((groups, width), jnp.int32)
    for g in range(groups):
        full_rows = jnp.where(group == g, full[g].astype(jnp.int32), full_rows)
    fill = jnp.zeros((groups, width - slots), jnp.int32)
    first = jnp.concatenate([dst_ref[pl.ds(0, groups, stride=2), :], fill], axis=1)
    second = jnp.concatenate([dst_ref[pl.ds(1, groups, stride=2), :], fill], axis=1) + owned
    by_half = pltpu.roll(second, half, 1)
    by_full = pltpu.roll(second, slots, 1)
    when_full = jnp.where(lane < slots, first, by_full)
    when_half = jnp.where(lane < half, first, by_half)
    labels = jnp.where(full_rows == 1, when_full, when_half).astype(jnp.float32)
    fetches[2].wait()
    for place, g in enumerate(order):
        base = place * pitch
        a0 = messages_ref[g, 0, :half, :]
        a1 = messages_ref[g, 0, half:, :]
        b0 = messages_ref[g, 1, :half, :]
        b1 = messages_ref[g, 1, half:, :]
        out_ref[base : base + half, :] = a0
        out_ref[base + half : base + slots, :] = jnp.where(full[g], a1, b0)
        out_ref[base + slots : base + live, :] = jnp.where(full[g], b0, b1)
        out_ref[base + live : base + pitch, :] = labels[g : g + 1, :]


def slot_values(rows, received_ref, both_ref, label_ref):
    width = received_ref.shape[1]
    pitch = received_ref.shape[0] // rows
    live = pitch - 1
    total = rows * live
    labels = received_ref[pl.ds(live, rows, stride=pitch), :].astype(jnp.int32)
    left = live
    while left:
        step = min(left, (width - 1) // (rows - 1))
        labels = pltpu.roll(labels, 0, 1, stride=step, stride_axis=0)
        left -= step
    place = lax.broadcasted_iota(jnp.int32, (rows, width), 0)
    lane = lax.broadcasted_iota(jnp.int32, (rows, width), 1)
    slot = lax.rem(lane - lax.rem(place * live, width) + width, width)
    position = place * live + slot
    parts = []
    for block in range(total // width):
        inside = (slot < live) & (position >= block * width) & (position < (block + 1) * width)
        parts.append(jnp.sum(jnp.where(inside, labels, 0), axis=0, keepdims=True))
    label = jnp.concatenate(parts, axis=1)
    values = jnp.concatenate([received_ref[p * pitch : p * pitch + live, :] for p in range(rows)], axis=0)
    high = values.astype(jnp.bfloat16)
    low = (values - high.astype(jnp.float32)).astype(jnp.bfloat16)
    both = jnp.concatenate([high, low], axis=1)
    both_ref[...] = both
    label_ref[...] = jnp.broadcast_to(label, label_ref.shape)
    return both, label


def range_sums(owned, side, both, label):
    width = both.shape[1] // 2
    vertex = lax.broadcasted_iota(jnp.int32, (owned, both.shape[0]), 0)
    hot = (vertex == label - side * owned).astype(jnp.float32).astype(jnp.bfloat16)
    sums = jnp.dot(hot, both, preferred_element_type=jnp.float32)
    return sums[:, :width] + sums[:, width:]


def other_kernel(rows, owned, received_ref, other_ref, both_ref, label_ref):
    both, label = slot_values(rows, received_ref, both_ref, label_ref)
    other_ref[...] = range_sums(owned, 1 - lax.axis_index("col"), both, label)


def own_kernel(owned, both_ref, label_ref, degrees_ref, own_ref, share_ref):
    width = own_ref.shape[1]
    sums = range_sums(owned, lax.axis_index("col"), both_ref[...], label_ref[0:1, :])
    for start in range(0, owned, width):
        scale = jnp.maximum(degrees_ref[0:1, start : start + width], 1).astype(jnp.float32)
        share = jnp.transpose(jnp.broadcast_to(1.0 / scale, (width, width)))
        share_ref[start : start + width, :] = share
        own_ref[start : start + width, :] = sums[start : start + width, :] * share


def last_kernel(pieces, own_ref, mine_ref, share_ref, out_hbm, out_ref, sems):
    size = out_ref.shape[0] // pieces
    copies = []
    for i in range(pieces):
        piece = slice(i * size, (i + 1) * size)
        out_ref[piece, :] = own_ref[piece, :] + mine_ref[piece, :] * share_ref[piece, :]
        copies.append(pltpu.make_async_copy(out_ref.at[piece, :], out_hbm.at[piece, :], sems.at[i]))
        copies[-1].start()
    for copy in copies:
        copy.wait()


def paired(rows, messages, dst_local, counts, degrees):
    _, groups, subs, slots, width = messages.shape
    owned = degrees.shape[0]
    pitch = slots + slots // 2 + 1
    order = meeting_order(rows)
    total = rows * (pitch - 1)
    vmem = pl.BlockSpec(memory_space=pltpu.VMEM)
    hbm = pl.BlockSpec(memory_space=pltpu.HBM)
    packed = pl.pallas_call(
        lambda *refs: pack_kernel(order, owned, *refs),
        out_shape=jax.ShapeDtypeStruct((groups * pitch, width), jnp.float32),
        in_specs=[hbm, hbm, hbm],
        out_specs=vmem,
        scratch_shapes=[
            pltpu.SMEM((subs, groups), jnp.int32),
            pltpu.VMEM((groups * subs, slots), jnp.int32),
            pltpu.VMEM((groups, subs, slots, width), jnp.float32),
            pltpu.SemaphoreType.DMA((3,)),
        ],
        compiler_params=SMALL,
        name="pack",
    )(in_hbm(counts.reshape(groups, subs).T), in_hbm(dst_local.reshape(groups * subs, slots)), in_hbm(messages[0]))
    received = lax.all_to_all(
        packed.reshape(groups * pitch, 1, width),
        ("row", "col"),
        split_axis=0,
        concat_axis=0,
        tiled=True,
        axis_index_groups=exchange_groups(order, 2),
    ).reshape(groups * pitch, width)
    partial = jax.ShapeDtypeStruct((owned, width), jnp.float32)
    other, both, label = pl.pallas_call(
        lambda *refs: other_kernel(rows, owned, *refs),
        out_shape=[
            partial,
            jax.ShapeDtypeStruct((total, 2 * width), jnp.bfloat16),
            jax.ShapeDtypeStruct((SUBLANES, total), jnp.int32),
        ],
        in_specs=[vmem],
        out_specs=[vmem] * 3,
        compiler_params=SMALL,
        name="other_sums",
    )(received)
    mine = lax.ppermute(other, "col", [(0, 1), (1, 0)])
    own, share = pl.pallas_call(
        lambda *refs: own_kernel(owned, *refs),
        out_shape=[partial, partial],
        in_specs=[vmem] * 3,
        out_specs=[vmem] * 2,
        compiler_params=SMALL,
        cost_estimate=pl.CostEstimate(flops=4 * owned * total * width, bytes_accessed=1 << 20, transcendentals=0),
        name="own_sums",
    )(both, label, degrees.reshape(1, owned))
    pieces = 4
    return pl.pallas_call(
        lambda *refs: last_kernel(pieces, *refs),
        out_shape=partial,
        in_specs=[vmem] * 3,
        out_specs=hbm,
        scratch_shapes=[pltpu.VMEM((owned, width), jnp.float32), pltpu.SemaphoreType.DMA((pieces,))],
        compiler_params=SMALL,
        name="mean",
    )(own, mine, share)


def solution(mesh):
    rows, cols = mesh.shape["row"], mesh.shape["col"]

    def body(messages, dst_local, counts, degrees):
        subs, slots, width = messages.shape[2:]
        live = slots + slots // 2
        fits = width == LANES and slots % (2 * SUBLANES) == 0 and rows * live % width == 0
        if subs == cols == 2 and fits and rows <= 16:
            return paired(rows, messages, dst_local, counts, degrees)
        return general(messages, dst_local, counts, degrees)

    in_specs = (
        P(("row", "col"), None, None, None, None),
        P(("row", "col"), None, None, None),
        P(("row", "col"), None, None),
        P(("row", "col")),
    )
    out_specs = P(("row", "col"), None)
    return jax.shard_map(body, mesh=mesh, in_specs=in_specs, out_specs=out_specs, check_vma=False)
```

```python
import jax
import jax.numpy as jnp
from jax import lax
from jax.experimental import pallas as pl
from jax.experimental.pallas import tpu as pltpu
from jax.sharding import PartitionSpec as P

LANES = 128
SUBLANES = 8
FETCHES = 4
SMALL = pltpu.CompilerParams(vmem_limit_bytes=8 << 20)


def general(messages, dst_local, counts, degrees):
    slots = messages.shape[3]
    width = messages.shape[4]
    owned = degrees.shape[0]
    slot_index = lax.broadcasted_iota(jnp.int32, counts.shape + (slots,), 3)
    alive_mask = (slot_index < counts[..., None]).astype(jnp.float32)
    masked = messages * alive_mask[..., None]

    def exchange(x):
        x = lax.all_to_all(x, "row", split_axis=1, concat_axis=0, tiled=True)
        return lax.all_to_all(x, "col", split_axis=2, concat_axis=1, tiled=True)

    received, labels = exchange(masked), exchange(dst_local)
    summed = jax.ops.segment_sum(received.reshape(-1, width), labels.reshape(-1), num_segments=owned)
    scale = jnp.maximum(degrees, 1).astype(jnp.float32)
    return summed / scale[:, None]


def in_hbm(x):
    return pltpu.with_memory_space_constraint(x, pltpu.HBM)


ORDERS = {16: (11, 8, 5, 3, 13, 14, 4, 2, 15, 12, 7, 9, 10, 1, 6, 0)}


def meeting_order(rows):
    first = rows * 3 // 4 - 1
    return ORDERS.get(rows, (first, *(r for r in range(1, rows) if r != first), 0))


def exchange_groups(order, cols):
    swap = [int(2 * r >= len(order)) for r in order]
    return [[r * cols + (c ^ s) for r, s in zip(order, swap)] for c in range(cols)]


def pack_kernel(order, *refs):
    counts_hbm, dst_hbm, degrees_hbm, messages_hbm, out_ref, share_ref = refs[:6]
    counts_ref, dst_ref, degrees_ref, messages_ref, sems = refs[6:]
    groups, _, slots, width = messages_ref.shape
    owned = degrees_ref.shape[1]
    small = 3
    pieces = sems.shape[0] - small
    size = groups // pieces
    sides = [(counts_hbm, counts_ref), (dst_hbm, dst_ref), (degrees_hbm, degrees_ref)]
    for i in range(pieces):
        piece = pl.ds(i * size, size)
        sides.append((messages_hbm.at[piece], messages_ref.at[piece]))
    fetches = [pltpu.make_async_copy(*side, sems.at[i]) for i, side in enumerate(sides)]
    for fetch in fetches:
        fetch.start()
    half = slots // 2
    live = slots + half
    pitch = live + 1
    row = lax.axis_index("row")
    place = sum(jnp.where(row == r, p, 0) for p, r in enumerate(order))
    lane = lax.broadcasted_iota(jnp.int32, (groups, width), 1)
    group = lax.broadcasted_iota(jnp.int32, (groups, width), 0)
    fill = jnp.zeros((groups, width - slots), jnp.int32)
    for fetch in fetches[:small]:
        fetch.wait()
    full = [counts_ref[0, g] == slots for g in range(groups)]
    full_rows = jnp.zeros((groups, width), jnp.int32)
    for g in range(groups):
        full_rows = jnp.where(group == g, full[g].astype(jnp.int32), full_rows)
    first = jnp.concatenate([dst_ref[pl.ds(0, groups, stride=2), :], fill], axis=1)
    second = jnp.concatenate([dst_ref[pl.ds(1, groups, stride=2), :], fill], axis=1) + owned
    by_half = pltpu.roll(second, half, 1)
    by_full = pltpu.roll(second, slots, 1)
    when_full = jnp.where(lane < slots, first, by_full)
    when_half = jnp.where(lane < half, first, by_half)
    labels = jnp.where(lane < live, jnp.where(full_rows == 1, when_full, when_half), 0)
    labels = pltpu.roll(labels.astype(jnp.float32), lax.rem(place * live, width), 1)
    for p, g in enumerate(order):
        out_ref[p * pitch + live : (p + 1) * pitch, :] = labels[g : g + 1, :]
    for start in range(0, owned, width):
        scale = jnp.maximum(degrees_ref[0:1, start : start + width], 1).astype(jnp.float32)
        share_ref[start : start + width, :] = jnp.transpose(jnp.broadcast_to(1.0 / scale, (width, width)))
    for g in range(groups):
        if g % size == 0:
            fetches[small + g // size].wait()
        base = order.index(g) * pitch
        a0 = messages_ref[g, 0, :half, :]
        a1 = messages_ref[g, 0, half:, :]
        b0 = messages_ref[g, 1, :half, :]
        b1 = messages_ref[g, 1, half:, :]
        out_ref[base : base + half, :] = a0
        out_ref[base + half : base + slots, :] = jnp.where(full[g], a1, b0)
        out_ref[base + slots : base + live, :] = jnp.where(full[g], b0, b1)


def slot_values(rows, received_ref, both_ref, label_ref):
    width = received_ref.shape[1]
    pitch = received_ref.shape[0] // rows
    live = pitch - 1
    total = rows * live
    labels = received_ref[pl.ds(live, rows, stride=pitch), :].astype(jnp.int32)
    place = lax.broadcasted_iota(jnp.int32, (rows, width), 0)
    lane = lax.broadcasted_iota(jnp.int32, (rows, width), 1)
    slot = lax.rem(lane - lax.rem(place * live, width) + width, width)
    position = place * live + slot
    parts = []
    for block in range(total // width):
        inside = (slot < live) & (position >= block * width) & (position < (block + 1) * width)
        parts.append(jnp.sum(jnp.where(inside, labels, 0), axis=0, keepdims=True))
    label = jnp.concatenate(parts, axis=1)
    values = jnp.concatenate([received_ref[p * pitch : p * pitch + live, :] for p in range(rows)], axis=0)
    high = values.astype(jnp.bfloat16)
    low = (values - high.astype(jnp.float32)).astype(jnp.bfloat16)
    both = jnp.concatenate([high, low], axis=1)
    both_ref[...] = both
    label_ref[...] = jnp.broadcast_to(label, label_ref.shape)
    return both, label


def range_sums(owned, side, both, label):
    width = both.shape[1] // 2
    vertex = lax.broadcasted_iota(jnp.int32, (owned, both.shape[0]), 0)
    hot = (vertex == label - side * owned).astype(jnp.float32).astype(jnp.bfloat16)
    sums = jnp.dot(hot, both, preferred_element_type=jnp.float32)
    return sums[:, :width] + sums[:, width:]


def other_kernel(rows, owned, received_ref, other_ref, both_ref, label_ref):
    both, label = slot_values(rows, received_ref, both_ref, label_ref)
    other_ref[...] = range_sums(owned, 1 - lax.axis_index("col"), both, label)


def own_kernel(owned, both_ref, label_ref, share_ref, own_ref):
    sums = range_sums(owned, lax.axis_index("col"), both_ref[...], label_ref[0:1, :])
    own_ref[...] = sums * share_ref[...]


def last_kernel(pieces, own_ref, mine_ref, share_ref, out_hbm, out_ref, sems):
    size = out_ref.shape[0] // pieces
    copies = []
    for i in range(pieces):
        piece = slice(i * size, (i + 1) * size)
        out_ref[piece, :] = own_ref[piece, :] + mine_ref[piece, :] * share_ref[piece, :]
        copies.append(pltpu.make_async_copy(out_ref.at[piece, :], out_hbm.at[piece, :], sems.at[i]))
        copies[-1].start()
    for copy in copies:
        copy.wait()


def paired(rows, messages, dst_local, counts, degrees):
    _, groups, subs, slots, width = messages.shape
    owned = degrees.shape[0]
    pitch = slots + slots // 2 + 1
    order = meeting_order(rows)
    total = rows * (pitch - 1)
    vmem = pl.BlockSpec(memory_space=pltpu.VMEM)
    hbm = pl.BlockSpec(memory_space=pltpu.HBM)
    partial = jax.ShapeDtypeStruct((owned, width), jnp.float32)
    packed, share = pl.pallas_call(
        lambda *refs: pack_kernel(order, *refs),
        out_shape=[jax.ShapeDtypeStruct((groups * pitch, width), jnp.float32), partial],
        in_specs=[hbm] * 4,
        out_specs=[vmem] * 2,
        scratch_shapes=[
            pltpu.SMEM((subs, groups), jnp.int32),
            pltpu.VMEM((groups * subs, slots), jnp.int32),
            pltpu.VMEM((1, owned), jnp.int32),
            pltpu.VMEM((groups, subs, slots, width), jnp.float32),
            pltpu.SemaphoreType.DMA((3 + FETCHES,)),
        ],
        compiler_params=SMALL,
        name="pack",
    )(
        in_hbm(counts.reshape(groups, subs).T),
        in_hbm(dst_local.reshape(groups * subs, slots)),
        in_hbm(degrees.reshape(1, owned)),
        in_hbm(messages[0]),
    )
    received = lax.all_to_all(
        packed.reshape(groups * pitch, 1, width),
        ("row", "col"),
        split_axis=0,
        concat_axis=0,
        tiled=True,
        axis_index_groups=exchange_groups(order, 2),
    ).reshape(groups * pitch, width)
    other, both, label = pl.pallas_call(
        lambda *refs: other_kernel(rows, owned, *refs),
        out_shape=[
            partial,
            jax.ShapeDtypeStruct((total, 2 * width), jnp.bfloat16),
            jax.ShapeDtypeStruct((SUBLANES, total), jnp.int32),
        ],
        in_specs=[vmem],
        out_specs=[vmem] * 3,
        compiler_params=SMALL,
        name="other_sums",
    )(received)
    mine = lax.ppermute(other, "col", [(0, 1), (1, 0)])
    own = pl.pallas_call(
        lambda *refs: own_kernel(owned, *refs),
        out_shape=partial,
        in_specs=[vmem] * 3,
        out_specs=vmem,
        compiler_params=SMALL,
        cost_estimate=pl.CostEstimate(flops=4 * owned * total * width, bytes_accessed=1 << 20, transcendentals=0),
        name="own_sums",
    )(both, label, share)
    pieces = 4
    return pl.pallas_call(
        lambda *refs: last_kernel(pieces, *refs),
        out_shape=partial,
        in_specs=[vmem] * 3,
        out_specs=hbm,
        scratch_shapes=[pltpu.VMEM((owned, width), jnp.float32), pltpu.SemaphoreType.DMA((pieces,))],
        compiler_params=SMALL,
        name="mean",
    )(own, mine, share)


def solution(mesh):
    rows, cols = mesh.shape["row"], mesh.shape["col"]

    def body(messages, dst_local, counts, degrees):
        subs, slots, width = messages.shape[2:]
        live = slots + slots // 2
        fits = width == LANES and slots % (2 * SUBLANES) == 0 and rows * live % width == 0
        if subs == cols == 2 and fits and rows <= 16:
            return paired(rows, messages, dst_local, counts, degrees)
        return general(messages, dst_local, counts, degrees)

    in_specs = (
        P(("row", "col"), None, None, None, None),
        P(("row", "col"), None, None, None),
        P(("row", "col"), None, None),
        P(("row", "col")),
    )
    out_specs = P(("row", "col"), None)
    return jax.shard_map(body, mesh=mesh, in_specs=in_specs, out_specs=out_specs, check_vma=False)
```

```python
import jax
import jax.numpy as jnp
from jax import lax
from jax.experimental import pallas as pl
from jax.experimental.pallas import tpu as pltpu
from jax.sharding import PartitionSpec as P

LANES = 128
SUBLANES = 8
FETCHES = 1
SMALL = pltpu.CompilerParams(vmem_limit_bytes=8 << 20)


def general(messages, dst_local, counts, degrees):
    slots = messages.shape[3]
    width = messages.shape[4]
    owned = degrees.shape[0]
    slot_index = lax.broadcasted_iota(jnp.int32, counts.shape + (slots,), 3)
    alive_mask = (slot_index < counts[..., None]).astype(jnp.float32)
    masked = messages * alive_mask[..., None]

    def exchange(x):
        x = lax.all_to_all(x, "row", split_axis=1, concat_axis=0, tiled=True)
        return lax.all_to_all(x, "col", split_axis=2, concat_axis=1, tiled=True)

    received, labels = exchange(masked), exchange(dst_local)
    summed = jax.ops.segment_sum(received.reshape(-1, width), labels.reshape(-1), num_segments=owned)
    scale = jnp.maximum(degrees, 1).astype(jnp.float32)
    return summed / scale[:, None]


def in_hbm(x):
    return pltpu.with_memory_space_constraint(x, pltpu.HBM)


TUNED = {
    16: (
        (
            (11, 8, 5, 3, 9, 10, 4, 2, 15, 12, 7, 14, 6, 1, 13, 0),
            (11, 8, 4, 5, 3, 6, 9, 2, 15, 12, 7, 14, 10, 1, 13, 0),
        ),
        (3, 8, 9, 10, 11, 12, 13, 14, 15),
    ),
}


def exchange_plan(rows):
    first = rows * 3 // 4 - 1
    order = (first, *(r for r in range(1, rows) if r != first), 0)
    return TUNED.get(rows, ((order, order), tuple(range(rows // 2, rows))))


def pick(index, values):
    return sum(jnp.where(index == i, v, 0) for i, v in enumerate(values) if v)


def pack_kernel(orders, swapped, *refs):
    counts_hbm, dst_hbm, degrees_hbm, messages_hbm, out_ref, share_ref = refs[:6]
    counts_ref, dst_ref, degrees_ref, messages_ref, sems = refs[6:]
    groups, _, slots, width = messages_ref.shape
    owned = degrees_ref.shape[1]
    small = 3
    pieces = sems.shape[0] - small
    size = groups // pieces
    sides = [(counts_hbm, counts_ref), (dst_hbm, dst_ref), (degrees_hbm, degrees_ref)]
    for i in range(pieces):
        piece = pl.ds(i * size, size)
        sides.append((messages_hbm.at[piece], messages_ref.at[piece]))
    fetches = [pltpu.make_async_copy(*side, sems.at[i]) for i, side in enumerate(sides)]
    for fetch in fetches:
        fetch.start()
    half = slots // 2
    live = slots + half
    pitch = live + 1
    row = lax.axis_index("row")
    second_group = lax.axis_index("col") ^ pick(row, [int(r in swapped) for r in range(groups)])
    places = [jnp.where(second_group == 1, orders[1].index(g), orders[0].index(g)) for g in range(groups)]
    place = pick(row, [orders[0].index(r) for r in range(groups)])
    place = jnp.where(second_group == 1, pick(row, [orders[1].index(r) for r in range(groups)]), place)
    lane = lax.broadcasted_iota(jnp.int32, (groups, width), 1)
    group = lax.broadcasted_iota(jnp.int32, (groups, width), 0)
    fill = jnp.zeros((groups, width - slots), jnp.int32)
    for fetch in fetches[:small]:
        fetch.wait()
    full = [counts_ref[0, g] == slots for g in range(groups)]
    full_rows = jnp.zeros((groups, width), jnp.int32)
    for g in range(groups):
        full_rows = jnp.where(group == g, full[g].astype(jnp.int32), full_rows)
    first = jnp.concatenate([dst_ref[pl.ds(0, groups, stride=2), :], fill], axis=1)
    second = jnp.concatenate([dst_ref[pl.ds(1, groups, stride=2), :], fill], axis=1) + owned
    by_half = pltpu.roll(second, half, 1)
    by_full = pltpu.roll(second, slots, 1)
    when_full = jnp.where(lane < slots, first, by_full)
    when_half = jnp.where(lane < half, first, by_half)
    labels = jnp.where(lane < live, jnp.where(full_rows == 1, when_full, when_half), 0)
    labels = pltpu.roll(labels.astype(jnp.float32), lax.rem(place * live, width), 1)
    for g in range(groups):
        out_ref[pl.ds(places[g] * pitch + live, 1), :] = labels[g : g + 1, :]
    for start in range(0, owned, width):
        scale = jnp.maximum(degrees_ref[0:1, start : start + width], 1).astype(jnp.float32)
        share_ref[start : start + width, :] = jnp.transpose(jnp.broadcast_to(1.0 / scale, (width, width)))
    for g in range(groups):
        if g % size == 0:
            fetches[small + g // size].wait()
        base = places[g] * pitch
        a0 = messages_ref[g, 0, :half, :]
        a1 = messages_ref[g, 0, half:, :]
        b0 = messages_ref[g, 1, :half, :]
        b1 = messages_ref[g, 1, half:, :]
        out_ref[pl.ds(base, half), :] = a0
        out_ref[pl.ds(base + half, half), :] = jnp.where(full[g], a1, b0)
        out_ref[pl.ds(base + slots, half), :] = jnp.where(full[g], b0, b1)


def slot_values(rows, received_ref):
    width = received_ref.shape[1]
    pitch = received_ref.shape[0] // rows
    live = pitch - 1
    total = rows * live
    labels = received_ref[pl.ds(live, rows, stride=pitch), :].astype(jnp.int32)
    place = lax.broadcasted_iota(jnp.int32, (rows, width), 0)
    lane = lax.broadcasted_iota(jnp.int32, (rows, width), 1)
    slot = lax.rem(lane - lax.rem(place * live, width) + width, width)
    position = place * live + slot
    parts = []
    for block in range(total // width):
        inside = (slot < live) & (position >= block * width) & (position < (block + 1) * width)
        parts.append(jnp.sum(jnp.where(inside, labels, 0), axis=0, keepdims=True))
    label = jnp.concatenate(parts, axis=1)
    values = jnp.concatenate([received_ref[p * pitch : p * pitch + live, :] for p in range(rows)], axis=0)
    high = values.astype(jnp.bfloat16)
    low = (values - high.astype(jnp.float32)).astype(jnp.bfloat16)
    return jnp.concatenate([high, low], axis=1), label


def range_sums(owned, side, both, label):
    width = both.shape[1] // 2
    vertex = lax.broadcasted_iota(jnp.int32, (owned, both.shape[0]), 0)
    hot = (vertex == label - side * owned).astype(jnp.float32).astype(jnp.bfloat16)
    sums = jnp.dot(hot, both, preferred_element_type=jnp.float32)
    return sums[:, :width] + sums[:, width:]


def other_kernel(rows, owned, received_ref, other_ref):
    other_ref[...] = range_sums(owned, 1 - lax.axis_index("col"), *slot_values(rows, received_ref))


def own_kernel(rows, owned, received_ref, share_ref, own_ref):
    sums = range_sums(owned, lax.axis_index("col"), *slot_values(rows, received_ref))
    own_ref[...] = sums * share_ref[...]


def paired(rows, messages, dst_local, counts, degrees):
    _, groups, subs, slots, width = messages.shape
    owned = degrees.shape[0]
    pitch = slots + slots // 2 + 1
    orders, swapped = exchange_plan(rows)
    members = [[r * subs + (c ^ int(r in swapped)) for r in order] for c, order in enumerate(orders)]
    total = rows * (pitch - 1)
    vmem = pl.BlockSpec(memory_space=pltpu.VMEM)
    hbm = pl.BlockSpec(memory_space=pltpu.HBM)
    partial = jax.ShapeDtypeStruct((owned, width), jnp.float32)
    packed, share = pl.pallas_call(
        lambda *refs: pack_kernel(orders, swapped, *refs),
        out_shape=[jax.ShapeDtypeStruct((groups * pitch, width), jnp.float32), partial],
        in_specs=[hbm] * 4,
        out_specs=[vmem] * 2,
        scratch_shapes=[
            pltpu.SMEM((subs, groups), jnp.int32),
            pltpu.VMEM((groups * subs, slots), jnp.int32),
            pltpu.VMEM((1, owned), jnp.int32),
            pltpu.VMEM((groups, subs, slots, width), jnp.float32),
            pltpu.SemaphoreType.DMA((3 + FETCHES,)),
        ],
        compiler_params=SMALL,
        name="pack",
    )(
        in_hbm(counts.reshape(groups, subs).T),
        in_hbm(dst_local.reshape(groups * subs, slots)),
        in_hbm(degrees.reshape(1, owned)),
        in_hbm(messages[0]),
    )
    received = lax.all_to_all(
        packed.reshape(groups * pitch, 1, width),
        ("row", "col"),
        split_axis=0,
        concat_axis=0,
        tiled=True,
        axis_index_groups=members,
    ).reshape(groups * pitch, width)
    other = pl.pallas_call(
        lambda *refs: other_kernel(rows, owned, *refs),
        out_shape=partial,
        in_specs=[vmem],
        out_specs=vmem,
        compiler_params=SMALL,
        name="other_sums",
    )(received)
    mine = lax.ppermute(other, "col", [(0, 1), (1, 0)])
    own = pl.pallas_call(
        lambda *refs: own_kernel(rows, owned, *refs),
        out_shape=partial,
        in_specs=[vmem] * 2,
        out_specs=vmem,
        compiler_params=SMALL,
        cost_estimate=pl.CostEstimate(flops=4 * owned * total * width, bytes_accessed=1 << 20, transcendentals=0),
        name="own_sums",
    )(received, share)
    return own + mine * share


def solution(mesh):
    rows, cols = mesh.shape["row"], mesh.shape["col"]

    def body(messages, dst_local, counts, degrees):
        subs, slots, width = messages.shape[2:]
        live = slots + slots // 2
        fits = width == LANES and slots % (2 * SUBLANES) == 0 and rows * live % width == 0
        if subs == cols == 2 and fits and rows <= 16:
            return paired(rows, messages, dst_local, counts, degrees)
        return general(messages, dst_local, counts, degrees)

    in_specs = (
        P(("row", "col"), None, None, None, None),
        P(("row", "col"), None, None, None),
        P(("row", "col"), None, None),
        P(("row", "col")),
    )
    out_specs = P(("row", "col"), None)
    return jax.shard_map(body, mesh=mesh, in_specs=in_specs, out_specs=out_specs, check_vma=False)
```

```python
import jax
import jax.numpy as jnp
from jax import lax
from jax.experimental import pallas as pl
from jax.experimental.pallas import tpu as pltpu
from jax.sharding import PartitionSpec as P

LANES = 128
SUBLANES = 8
FETCHES = 1
SMALL = pltpu.CompilerParams(vmem_limit_bytes=8 << 20)


def general(messages, dst_local, counts, degrees):
    slots = messages.shape[3]
    width = messages.shape[4]
    owned = degrees.shape[0]
    slot_index = lax.broadcasted_iota(jnp.int32, counts.shape + (slots,), 3)
    alive_mask = (slot_index < counts[..., None]).astype(jnp.float32)
    masked = messages * alive_mask[..., None]

    def exchange(x):
        x = lax.all_to_all(x, "row", split_axis=1, concat_axis=0, tiled=True)
        return lax.all_to_all(x, "col", split_axis=2, concat_axis=1, tiled=True)

    received, labels = exchange(masked), exchange(dst_local)
    summed = jax.ops.segment_sum(received.reshape(-1, width), labels.reshape(-1), num_segments=owned)
    scale = jnp.maximum(degrees, 1).astype(jnp.float32)
    return summed / scale[:, None]


def in_hbm(x):
    return pltpu.with_memory_space_constraint(x, pltpu.HBM)


TUNED = {
    16: (
        (11, 8, 5, 3, 9, 10, 4, 2, 15, 12, 7, 14, 6, 1, 13, 0),
        (11, 2, 5, 3, 4, 6, 9, 8, 15, 12, 7, 14, 10, 1, 13, 0),
    ),
}


def exchange_plan(rows):
    first = rows * 3 // 4 - 1
    order = (first, *(r for r in range(1, rows) if r != first), 0)
    return TUNED.get(rows, (order, order)), range(rows // 2, rows)


def pick(index, values):
    return sum(jnp.where(index == i, v, 0) for i, v in enumerate(values) if v)


def pack_kernel(orders, swapped, *refs):
    counts_hbm, dst_hbm, degrees_hbm, messages_hbm, out_ref, share_ref = refs[:6]
    counts_ref, dst_ref, degrees_ref, messages_ref, sems = refs[6:]
    groups, _, slots, width = messages_ref.shape
    owned = degrees_ref.shape[1]
    small = 3
    pieces = sems.shape[0] - small
    size = groups // pieces
    sides = [(counts_hbm, counts_ref), (dst_hbm, dst_ref), (degrees_hbm, degrees_ref)]
    for i in range(pieces):
        piece = pl.ds(i * size, size)
        sides.append((messages_hbm.at[piece], messages_ref.at[piece]))
    fetches = [pltpu.make_async_copy(*side, sems.at[i]) for i, side in enumerate(sides)]
    for fetch in fetches:
        fetch.start()
    half = slots // 2
    live = slots + half
    pitch = live + 1
    row = lax.axis_index("row")
    second_group = lax.axis_index("col") ^ pick(row, [int(r in swapped) for r in range(groups)])
    places = [jnp.where(second_group == 1, orders[1].index(g), orders[0].index(g)) for g in range(groups)]
    place = pick(row, [orders[0].index(r) for r in range(groups)])
    place = jnp.where(second_group == 1, pick(row, [orders[1].index(r) for r in range(groups)]), place)
    lane = lax.broadcasted_iota(jnp.int32, (groups, width), 1)
    group = lax.broadcasted_iota(jnp.int32, (groups, width), 0)
    fill = jnp.zeros((groups, width - slots), jnp.int32)
    for fetch in fetches[:small]:
        fetch.wait()
    full = [counts_ref[0, g] == slots for g in range(groups)]
    full_rows = jnp.zeros((groups, width), jnp.int32)
    for g in range(groups):
        full_rows = jnp.where(group == g, full[g].astype(jnp.int32), full_rows)
    first = jnp.concatenate([dst_ref[pl.ds(0, groups, stride=2), :], fill], axis=1)
    second = jnp.concatenate([dst_ref[pl.ds(1, groups, stride=2), :], fill], axis=1) + owned
    by_half = pltpu.roll(second, half, 1)
    by_full = pltpu.roll(second, slots, 1)
    when_full = jnp.where(lane < slots, first, by_full)
    when_half = jnp.where(lane < half, first, by_half)
    labels = jnp.where(lane < live, jnp.where(full_rows == 1, when_full, when_half), 0)
    labels = pltpu.roll(labels.astype(jnp.float32), lax.rem(place * live, width), 1)
    for g in range(groups):
        out_ref[pl.ds(places[g] * pitch + live, 1), :] = labels[g : g + 1, :]
    for start in range(0, owned, width):
        scale = jnp.maximum(degrees_ref[0:1, start : start + width], 1).astype(jnp.float32)
        share_ref[start : start + width, :] = jnp.transpose(jnp.broadcast_to(1.0 / scale, (width, width)))
    for g in range(groups):
        if g % size == 0:
            fetches[small + g // size].wait()
        base = places[g] * pitch
        a0 = messages_ref[g, 0, :half, :]
        a1 = messages_ref[g, 0, half:, :]
        b0 = messages_ref[g, 1, :half, :]
        b1 = messages_ref[g, 1, half:, :]
        out_ref[pl.ds(base, half), :] = a0
        out_ref[pl.ds(base + half, half), :] = jnp.where(full[g], a1, b0)
        out_ref[pl.ds(base + slots, half), :] = jnp.where(full[g], b0, b1)


def slot_values(rows, received_ref):
    width = received_ref.shape[1]
    pitch = received_ref.shape[0] // rows
    live = pitch - 1
    total = rows * live
    labels = received_ref[pl.ds(live, rows, stride=pitch), :].astype(jnp.int32)
    place = lax.broadcasted_iota(jnp.int32, (rows, width), 0)
    lane = lax.broadcasted_iota(jnp.int32, (rows, width), 1)
    slot = lax.rem(lane - lax.rem(place * live, width) + width, width)
    position = place * live + slot
    parts = []
    for block in range(total // width):
        inside = (slot < live) & (position >= block * width) & (position < (block + 1) * width)
        parts.append(jnp.sum(jnp.where(inside, labels, 0), axis=0, keepdims=True))
    label = jnp.concatenate(parts, axis=1)
    values = jnp.concatenate([received_ref[p * pitch : p * pitch + live, :] for p in range(rows)], axis=0)
    high = values.astype(jnp.bfloat16)
    low = (values - high.astype(jnp.float32)).astype(jnp.bfloat16)
    return jnp.concatenate([high, low], axis=1), label


def range_sums(owned, side, both, label):
    width = both.shape[1] // 2
    vertex = lax.broadcasted_iota(jnp.int32, (owned, both.shape[0]), 0)
    hot = (vertex == label - side * owned).astype(jnp.float32).astype(jnp.bfloat16)
    sums = jnp.dot(hot, both, preferred_element_type=jnp.float32)
    return sums[:, :width] + sums[:, width:]


def other_kernel(rows, owned, received_ref, other_ref):
    other_ref[...] = range_sums(owned, 1 - lax.axis_index("col"), *slot_values(rows, received_ref))


def own_kernel(rows, owned, received_ref, share_ref, own_ref):
    sums = range_sums(owned, lax.axis_index("col"), *slot_values(rows, received_ref))
    own_ref[...] = sums * share_ref[...]


def paired(rows, messages, dst_local, counts, degrees):
    _, groups, subs, slots, width = messages.shape
    owned = degrees.shape[0]
    pitch = slots + slots // 2 + 1
    orders, swapped = exchange_plan(rows)
    members = [[r * subs + (c ^ int(r in swapped)) for r in order] for c, order in enumerate(orders)]
    total = rows * (pitch - 1)
    vmem = pl.BlockSpec(memory_space=pltpu.VMEM)
    hbm = pl.BlockSpec(memory_space=pltpu.HBM)
    partial = jax.ShapeDtypeStruct((owned, width), jnp.float32)
    packed, share = pl.pallas_call(
        lambda *refs: pack_kernel(orders, swapped, *refs),
        out_shape=[jax.ShapeDtypeStruct((groups * pitch, width), jnp.float32), partial],
        in_specs=[hbm] * 4,
        out_specs=[vmem] * 2,
        scratch_shapes=[
            pltpu.SMEM((subs, groups), jnp.int32),
            pltpu.VMEM((groups * subs, slots), jnp.int32),
            pltpu.VMEM((1, owned), jnp.int32),
            pltpu.VMEM((groups, subs, slots, width), jnp.float32),
            pltpu.SemaphoreType.DMA((3 + FETCHES,)),
        ],
        compiler_params=SMALL,
        name="pack",
    )(
        in_hbm(counts.reshape(groups, subs).T),
        in_hbm(dst_local.reshape(groups * subs, slots)),
        in_hbm(degrees.reshape(1, owned)),
        in_hbm(messages[0]),
    )
    received = lax.all_to_all(
        packed.reshape(groups * pitch, 1, width),
        ("row", "col"),
        split_axis=0,
        concat_axis=0,
        tiled=True,
        axis_index_groups=members,
    ).reshape(groups * pitch, width)
    other = pl.pallas_call(
        lambda *refs: other_kernel(rows, owned, *refs),
        out_shape=partial,
        in_specs=[vmem],
        out_specs=vmem,
        compiler_params=SMALL,
        name="other_sums",
    )(received)
    mine = lax.ppermute(other, "col", [(0, 1), (1, 0)])
    own = pl.pallas_call(
        lambda *refs: own_kernel(rows, owned, *refs),
        out_shape=partial,
        in_specs=[vmem] * 2,
        out_specs=vmem,
        compiler_params=SMALL,
        cost_estimate=pl.CostEstimate(flops=4 * owned * total * width, bytes_accessed=1 << 20, transcendentals=0),
        name="own_sums",
    )(received, share)
    return own + mine * share


def solution(mesh):
    rows, cols = mesh.shape["row"], mesh.shape["col"]

    def body(messages, dst_local, counts, degrees):
        subs, slots, width = messages.shape[2:]
        live = slots + slots // 2
        fits = width == LANES and slots % (2 * SUBLANES) == 0 and rows * live % width == 0
        if subs == cols == 2 and fits and rows <= 16:
            return paired(rows, messages, dst_local, counts, degrees)
        return general(messages, dst_local, counts, degrees)

    in_specs = (
        P(("row", "col"), None, None, None, None),
        P(("row", "col"), None, None, None),
        P(("row", "col"), None, None),
        P(("row", "col")),
    )
    out_specs = P(("row", "col"), None)
    return jax.shard_map(body, mesh=mesh, in_specs=in_specs, out_specs=out_specs, check_vma=False)
```

```python
import jax
import jax.numpy as jnp
from jax import lax
from jax.experimental import pallas as pl
from jax.experimental.pallas import tpu as pltpu
from jax.sharding import PartitionSpec as P

LANES = 128
SUBLANES = 8
FETCHES = 1
SMALL = pltpu.CompilerParams(vmem_limit_bytes=8 << 20)


def general(messages, dst_local, counts, degrees):
    slots = messages.shape[3]
    width = messages.shape[4]
    owned = degrees.shape[0]
    slot_index = lax.broadcasted_iota(jnp.int32, counts.shape + (slots,), 3)
    alive_mask = (slot_index < counts[..., None]).astype(jnp.float32)
    masked = messages * alive_mask[..., None]

    def exchange(x):
        x = lax.all_to_all(x, "row", split_axis=1, concat_axis=0, tiled=True)
        return lax.all_to_all(x, "col", split_axis=2, concat_axis=1, tiled=True)

    received, labels = exchange(masked), exchange(dst_local)
    summed = jax.ops.segment_sum(received.reshape(-1, width), labels.reshape(-1), num_segments=owned)
    scale = jnp.maximum(degrees, 1).astype(jnp.float32)
    return summed / scale[:, None]


def in_hbm(x):
    return pltpu.with_memory_space_constraint(x, pltpu.HBM)


TUNED = {
    16: (
        (11, 8, 5, 3, 9, 10, 4, 2, 15, 12, 7, 14, 6, 1, 13, 0),
        (11, 2, 5, 3, 4, 6, 9, 8, 15, 12, 7, 14, 10, 1, 13, 0),
    ),
}


def exchange_plan(rows):
    first = rows * 3 // 4 - 1
    order = (first, *(r for r in range(1, rows) if r != first), 0)
    return TUNED.get(rows, (order, order)), range(rows // 2, rows)


def pick(index, values):
    return sum(jnp.where(index == i, v, 0) for i, v in enumerate(values) if v)


def pack_kernel(orders, swapped, *refs):
    counts_hbm, dst_hbm, degrees_hbm, messages_hbm, out_ref, share_ref = refs[:6]
    counts_ref, dst_ref, degrees_ref, messages_ref, sems = refs[6:]
    groups, _, slots, width = messages_ref.shape
    owned = degrees_ref.shape[1]
    small = 3
    pieces = sems.shape[0] - small
    size = groups // pieces
    sides = [(counts_hbm, counts_ref), (dst_hbm, dst_ref), (degrees_hbm, degrees_ref)]
    for i in range(pieces):
        piece = pl.ds(i * size, size)
        sides.append((messages_hbm.at[piece], messages_ref.at[piece]))
    fetches = [pltpu.make_async_copy(*side, sems.at[i]) for i, side in enumerate(sides)]
    for fetch in fetches:
        fetch.start()
    half = slots // 2
    live = slots + half
    pitch = live + 1
    row = lax.axis_index("row")
    second_group = lax.axis_index("col") ^ pick(row, [int(r in swapped) for r in range(groups)])
    places = [jnp.where(second_group == 1, orders[1].index(g), orders[0].index(g)) for g in range(groups)]
    place = pick(row, [orders[0].index(r) for r in range(groups)])
    place = jnp.where(second_group == 1, pick(row, [orders[1].index(r) for r in range(groups)]), place)
    lane = lax.broadcasted_iota(jnp.int32, (groups, width), 1)
    group = lax.broadcasted_iota(jnp.int32, (groups, width), 0)
    fill = jnp.zeros((groups, width - slots), jnp.int32)
    for fetch in fetches[:small]:
        fetch.wait()
    full = [counts_ref[0, g] == slots for g in range(groups)]
    full_rows = jnp.zeros((groups, width), jnp.int32)
    for g in range(groups):
        full_rows = jnp.where(group == g, full[g].astype(jnp.int32), full_rows)
    first = jnp.concatenate([dst_ref[pl.ds(0, groups, stride=2), :], fill], axis=1)
    second = jnp.concatenate([dst_ref[pl.ds(1, groups, stride=2), :], fill], axis=1) + owned
    by_half = pltpu.roll(second, half, 1)
    by_full = pltpu.roll(second, slots, 1)
    when_full = jnp.where(lane < slots, first, by_full)
    when_half = jnp.where(lane < half, first, by_half)
    labels = jnp.where(lane < live, jnp.where(full_rows == 1, when_full, when_half), 0)
    labels = pltpu.roll(labels.astype(jnp.float32), lax.rem(place * live, width), 1)
    for g in range(groups):
        out_ref[pl.ds(places[g] * pitch + live, 1), :] = labels[g : g + 1, :]
    for start in range(0, owned, width):
        scale = jnp.maximum(degrees_ref[0:1, start : start + width], 1).astype(jnp.float32)
        share_ref[start : start + width, :] = jnp.transpose(jnp.broadcast_to(1.0 / scale, (width, width)))
    for g in range(groups):
        if g % size == 0:
            fetches[small + g // size].wait()
        base = places[g] * pitch
        a0 = messages_ref[g, 0, :half, :]
        a1 = messages_ref[g, 0, half:, :]
        b0 = messages_ref[g, 1, :half, :]
        b1 = messages_ref[g, 1, half:, :]
        out_ref[pl.ds(base, half), :] = a0
        out_ref[pl.ds(base + half, half), :] = jnp.where(full[g], a1, b0)
        out_ref[pl.ds(base + slots, half), :] = jnp.where(full[g], b0, b1)


def slot_values(rows, received_ref):
    width = received_ref.shape[1]
    pitch = received_ref.shape[0] // rows
    live = pitch - 1
    total = rows * live
    labels = received_ref[pl.ds(live, rows, stride=pitch), :].astype(jnp.int32)
    place = lax.broadcasted_iota(jnp.int32, (rows, width), 0)
    lane = lax.broadcasted_iota(jnp.int32, (rows, width), 1)
    slot = lax.rem(lane - lax.rem(place * live, width) + width, width)
    position = place * live + slot
    parts = []
    for block in range(total // width):
        inside = (slot < live) & (position >= block * width) & (position < (block + 1) * width)
        parts.append(jnp.sum(jnp.where(inside, labels, 0), axis=0, keepdims=True))
    label = jnp.concatenate(parts, axis=1)
    values = jnp.concatenate([received_ref[p * pitch : p * pitch + live, :] for p in range(rows)], axis=0)
    high = values.astype(jnp.bfloat16)
    low = (values - high.astype(jnp.float32)).astype(jnp.bfloat16)
    return jnp.concatenate([high, low], axis=1), label


def range_sums(owned, side, both, label):
    width = both.shape[1] // 2
    vertex = lax.broadcasted_iota(jnp.int32, (owned, both.shape[0]), 0)
    hot = (vertex == label - side * owned).astype(jnp.float32).astype(jnp.bfloat16)
    sums = jnp.dot(hot, both, preferred_element_type=jnp.float32)
    return sums[:, :width] + sums[:, width:]


def own_kernel(rows, owned, received_ref, share_ref, own_ref):
    sums = range_sums(owned, lax.axis_index("col"), *slot_values(rows, received_ref))
    own_ref[...] = sums * share_ref[...]


def last_kernel(rows, owned, received_ref, own_ref, share_ref, out_hbm, out_ref, sems):
    both, label = slot_values(rows, received_ref)
    width = out_ref.shape[1]
    parts = sems.shape[0]
    size = owned // parts
    copies = []
    for i in range(parts):
        part = pl.ds(i * size, size)
        vertex = lax.broadcasted_iota(jnp.int32, (size, both.shape[0]), 0) + i * size
        hot = (vertex == label - lax.axis_index("col") * owned).astype(jnp.float32).astype(jnp.bfloat16)
        sums = jnp.dot(hot, both, preferred_element_type=jnp.float32)
        out_ref[part, :] = own_ref[part, :] + (sums[:, :width] + sums[:, width:]) * share_ref[part, :]
        copies.append(pltpu.make_async_copy(out_ref.at[part, :], out_hbm.at[part, :], sems.at[i]))
        copies[-1].start()
    for copy in copies:
        copy.wait()


def paired(rows, messages, dst_local, counts, degrees):
    _, groups, subs, slots, width = messages.shape
    owned = degrees.shape[0]
    pitch = slots + slots // 2 + 1
    orders, swapped = exchange_plan(rows)
    members = [[r * subs + (c ^ int(r in swapped)) for r in order] for c, order in enumerate(orders)]
    total = rows * (pitch - 1)
    vmem = pl.BlockSpec(memory_space=pltpu.VMEM)
    hbm = pl.BlockSpec(memory_space=pltpu.HBM)
    partial = jax.ShapeDtypeStruct((owned, width), jnp.float32)
    packed, share = pl.pallas_call(
        lambda *refs: pack_kernel(orders, swapped, *refs),
        out_shape=[jax.ShapeDtypeStruct((groups * pitch, width), jnp.float32), partial],
        in_specs=[hbm] * 4,
        out_specs=[vmem] * 2,
        scratch_shapes=[
            pltpu.SMEM((subs, groups), jnp.int32),
            pltpu.VMEM((groups * subs, slots), jnp.int32),
            pltpu.VMEM((1, owned), jnp.int32),
            pltpu.VMEM((groups, subs, slots, width), jnp.float32),
            pltpu.SemaphoreType.DMA((3 + FETCHES,)),
        ],
        compiler_params=SMALL,
        name="pack",
    )(
        in_hbm(counts.reshape(groups, subs).T),
        in_hbm(dst_local.reshape(groups * subs, slots)),
        in_hbm(degrees.reshape(1, owned)),
        in_hbm(messages[0]),
    )
    received = lax.all_to_all(
        packed.reshape(groups * pitch, 1, width),
        ("row", "col"),
        split_axis=0,
        concat_axis=0,
        tiled=True,
        axis_index_groups=members,
    ).reshape(groups * pitch, width)
    crossed = lax.ppermute(received, "col", [(0, 1), (1, 0)])
    own = pl.pallas_call(
        lambda *refs: own_kernel(rows, owned, *refs),
        out_shape=partial,
        in_specs=[vmem] * 2,
        out_specs=vmem,
        compiler_params=SMALL,
        cost_estimate=pl.CostEstimate(flops=4 * owned * total * width, bytes_accessed=1 << 20, transcendentals=0),
        name="own_sums",
    )(received, share)
    parts = 2
    return pl.pallas_call(
        lambda *refs: last_kernel(rows, owned, *refs),
        out_shape=partial,
        in_specs=[vmem] * 3,
        out_specs=hbm,
        scratch_shapes=[pltpu.VMEM((owned, width), jnp.float32), pltpu.SemaphoreType.DMA((parts,))],
        compiler_params=SMALL,
        name="last_sums",
    )(crossed, own, share)


def solution(mesh):
    rows, cols = mesh.shape["row"], mesh.shape["col"]

    def body(messages, dst_local, counts, degrees):
        subs, slots, width = messages.shape[2:]
        live = slots + slots // 2
        fits = width == LANES and slots % (2 * SUBLANES) == 0 and rows * live % width == 0
        if subs == cols == 2 and fits and rows <= 16:
            return paired(rows, messages, dst_local, counts, degrees)
        return general(messages, dst_local, counts, degrees)

    in_specs = (
        P(("row", "col"), None, None, None, None),
        P(("row", "col"), None, None, None),
        P(("row", "col"), None, None),
        P(("row", "col")),
    )
    out_specs = P(("row", "col"), None)
    return jax.shard_map(body, mesh=mesh, in_specs=in_specs, out_specs=out_specs, check_vma=False)
```

```python
import jax
import jax.numpy as jnp
from jax import lax
from jax.experimental import pallas as pl
from jax.experimental.pallas import tpu as pltpu
from jax.sharding import PartitionSpec as P

LANES = 128
SUBLANES = 8
FETCHES = 1
SMALL = pltpu.CompilerParams(vmem_limit_bytes=8 << 20)


def general(messages, dst_local, counts, degrees):
    slots = messages.shape[3]
    width = messages.shape[4]
    owned = degrees.shape[0]
    slot_index = lax.broadcasted_iota(jnp.int32, counts.shape + (slots,), 3)
    alive_mask = (slot_index < counts[..., None]).astype(jnp.float32)
    masked = messages * alive_mask[..., None]

    def exchange(x):
        x = lax.all_to_all(x, "row", split_axis=1, concat_axis=0, tiled=True)
        return lax.all_to_all(x, "col", split_axis=2, concat_axis=1, tiled=True)

    received, labels = exchange(masked), exchange(dst_local)
    summed = jax.ops.segment_sum(received.reshape(-1, width), labels.reshape(-1), num_segments=owned)
    scale = jnp.maximum(degrees, 1).astype(jnp.float32)
    return summed / scale[:, None]


def in_hbm(x):
    return pltpu.with_memory_space_constraint(x, pltpu.HBM)


TUNED = {
    16: (
        (11, 8, 5, 3, 9, 10, 4, 2, 15, 12, 7, 14, 6, 1, 13, 0),
        (11, 2, 5, 3, 4, 6, 9, 8, 15, 12, 7, 14, 10, 1, 13, 0),
    ),
}


def exchange_plan(rows):
    first = rows * 3 // 4 - 1
    order = (first, *(r for r in range(1, rows) if r != first), 0)
    return TUNED.get(rows, (order, order)), range(rows // 2, rows)


def pick(index, values):
    return sum(jnp.where(index == i, v, 0) for i, v in enumerate(values) if v)


def pack_kernel(orders, swapped, *refs):
    counts_hbm, dst_hbm, degrees_hbm, messages_hbm, out_ref, share_ref = refs[:6]
    counts_ref, dst_ref, degrees_ref, messages_ref, sems = refs[6:]
    groups, _, slots, width = messages_ref.shape
    owned = degrees_ref.shape[1]
    small = 3
    pieces = sems.shape[0] - small
    size = groups // pieces
    sides = [(counts_hbm, counts_ref), (dst_hbm, dst_ref), (degrees_hbm, degrees_ref)]
    for i in range(pieces):
        piece = pl.ds(i * size, size)
        sides.append((messages_hbm.at[piece], messages_ref.at[piece]))
    fetches = [pltpu.make_async_copy(*side, sems.at[i]) for i, side in enumerate(sides)]
    for fetch in fetches:
        fetch.start()
    half = slots // 2
    live = slots + half
    pitch = live + 1
    row = lax.axis_index("row")
    second_group = lax.axis_index("col") ^ pick(row, [int(r in swapped) for r in range(groups)])
    places = [jnp.where(second_group == 1, orders[1].index(g), orders[0].index(g)) for g in range(groups)]
    place = pick(row, [orders[0].index(r) for r in range(groups)])
    place = jnp.where(second_group == 1, pick(row, [orders[1].index(r) for r in range(groups)]), place)
    lane = lax.broadcasted_iota(jnp.int32, (groups, width), 1)
    group = lax.broadcasted_iota(jnp.int32, (groups, width), 0)
    fill = jnp.zeros((groups, width - slots), jnp.int32)
    for fetch in fetches[:small]:
        fetch.wait()
    full = [counts_ref[0, g] == slots for g in range(groups)]
    full_rows = jnp.zeros((groups, width), jnp.int32)
    for g in range(groups):
        full_rows = jnp.where(group == g, full[g].astype(jnp.int32), full_rows)
    first = jnp.concatenate([dst_ref[pl.ds(0, groups, stride=2), :], fill], axis=1)
    second = jnp.concatenate([dst_ref[pl.ds(1, groups, stride=2), :], fill], axis=1) + owned
    by_half = pltpu.roll(second, half, 1)
    by_full = pltpu.roll(second, slots, 1)
    when_full = jnp.where(lane < slots, first, by_full)
    when_half = jnp.where(lane < half, first, by_half)
    labels = jnp.where(lane < live, jnp.where(full_rows == 1, when_full, when_half), 0)
    labels = pltpu.roll(labels.astype(jnp.float32), lax.rem(place * slots, width), 1)
    for g in range(groups):
        out_ref[pl.ds(places[g] * pitch + live, 1), :] = labels[g : g + 1, :]
    for start in range(0, owned, width):
        scale = jnp.maximum(degrees_ref[0:1, start : start + width], 1).astype(jnp.float32)
        share_ref[start : start + width, :] = jnp.transpose(jnp.broadcast_to(1.0 / scale, (width, width)))
    for g in range(groups):
        if g % size == 0:
            fetches[small + g // size].wait()
        base = places[g] * pitch
        a0 = messages_ref[g, 0, :half, :]
        a1 = messages_ref[g, 0, half:, :]
        b0 = messages_ref[g, 1, :half, :]
        b1 = messages_ref[g, 1, half:, :]
        out_ref[pl.ds(base, half), :] = a0
        out_ref[pl.ds(base + half, half), :] = jnp.where(full[g], a1, b0)
        out_ref[pl.ds(base + slots, half), :] = jnp.where(full[g], b0, b1)


def slot_values(rows, side, received_ref):
    width = received_ref.shape[1]
    pitch = received_ref.shape[0] // rows
    live = pitch - 1
    half = live // 3
    window = 2 * half
    labels = received_ref[pl.ds(live, rows, stride=pitch), :].astype(jnp.int32)
    labels = pltpu.roll(labels, jnp.where(side == 1, width - half, 0), 1)
    place = lax.broadcasted_iota(jnp.int32, (rows, width), 0)
    lane = lax.broadcasted_iota(jnp.int32, (rows, width), 1)
    position = place * window + lax.rem(lane - lax.rem(place * window, width) + width, width)
    inside = position < (place + 1) * window
    parts = []
    for block in range(rows * window // width):
        here = inside & (position >= block * width) & (position < (block + 1) * width)
        parts.append(jnp.sum(jnp.where(here, labels, 0), axis=0, keepdims=True))
    label = jnp.concatenate(parts, axis=1)
    first = side * half
    values = jnp.concatenate([received_ref[pl.ds(p * pitch + first, window), :] for p in range(rows)], axis=0)
    high = values.astype(jnp.bfloat16)
    low = (values - high.astype(jnp.float32)).astype(jnp.bfloat16)
    return jnp.concatenate([high, low], axis=1), label


def range_sums(owned, side, both, label):
    width = both.shape[1] // 2
    vertex = lax.broadcasted_iota(jnp.int32, (owned, both.shape[0]), 0)
    hot = (vertex == label - side * owned).astype(jnp.float32).astype(jnp.bfloat16)
    sums = jnp.dot(hot, both, preferred_element_type=jnp.float32)
    return sums[:, :width] + sums[:, width:]


def side_sums(rows, owned, side, received_ref):
    return range_sums(owned, side, *slot_values(rows, side, received_ref))


def other_kernel(rows, owned, received_ref, other_ref):
    other_ref[...] = side_sums(rows, owned, 1 - lax.axis_index("col"), received_ref)


def own_kernel(rows, owned, received_ref, share_ref, own_ref):
    sums = side_sums(rows, owned, lax.axis_index("col"), received_ref)
    own_ref[...] = sums * share_ref[...]


def paired(rows, messages, dst_local, counts, degrees):
    _, groups, subs, slots, width = messages.shape
    owned = degrees.shape[0]
    pitch = slots + slots // 2 + 1
    orders, swapped = exchange_plan(rows)
    members = [[r * subs + (c ^ int(r in swapped)) for r in order] for c, order in enumerate(orders)]
    total = rows * slots
    vmem = pl.BlockSpec(memory_space=pltpu.VMEM)
    hbm = pl.BlockSpec(memory_space=pltpu.HBM)
    partial = jax.ShapeDtypeStruct((owned, width), jnp.float32)
    packed, share = pl.pallas_call(
        lambda *refs: pack_kernel(orders, swapped, *refs),
        out_shape=[jax.ShapeDtypeStruct((groups * pitch, width), jnp.float32), partial],
        in_specs=[hbm] * 4,
        out_specs=[vmem] * 2,
        scratch_shapes=[
            pltpu.SMEM((subs, groups), jnp.int32),
            pltpu.VMEM((groups * subs, slots), jnp.int32),
            pltpu.VMEM((1, owned), jnp.int32),
            pltpu.VMEM((groups, subs, slots, width), jnp.float32),
            pltpu.SemaphoreType.DMA((3 + FETCHES,)),
        ],
        compiler_params=SMALL,
        name="pack",
    )(
        in_hbm(counts.reshape(groups, subs).T),
        in_hbm(dst_local.reshape(groups * subs, slots)),
        in_hbm(degrees.reshape(1, owned)),
        in_hbm(messages[0]),
    )
    received = lax.all_to_all(
        packed.reshape(groups * pitch, 1, width),
        ("row", "col"),
        split_axis=0,
        concat_axis=0,
        tiled=True,
        axis_index_groups=members,
    ).reshape(groups * pitch, width)
    other = pl.pallas_call(
        lambda *refs: other_kernel(rows, owned, *refs),
        out_shape=partial,
        in_specs=[vmem],
        out_specs=vmem,
        compiler_params=SMALL,
        name="other_sums",
    )(received)
    mine = lax.ppermute(other, "col", [(0, 1), (1, 0)])
    own = pl.pallas_call(
        lambda *refs: own_kernel(rows, owned, *refs),
        out_shape=partial,
        in_specs=[vmem] * 2,
        out_specs=vmem,
        compiler_params=SMALL,
        cost_estimate=pl.CostEstimate(flops=4 * owned * total * width, bytes_accessed=1 << 20, transcendentals=0),
        name="own_sums",
    )(received, share)
    return own + mine * share


def solution(mesh):
    rows, cols = mesh.shape["row"], mesh.shape["col"]

    def body(messages, dst_local, counts, degrees):
        subs, slots, width = messages.shape[2:]
        fits = width == LANES and slots % (2 * SUBLANES) == 0 and rows * slots % width == 0
        if subs == cols == 2 and fits and rows <= 16:
            return paired(rows, messages, dst_local, counts, degrees)
        return general(messages, dst_local, counts, degrees)

    in_specs = (
        P(("row", "col"), None, None, None, None),
        P(("row", "col"), None, None, None),
        P(("row", "col"), None, None),
        P(("row", "col")),
    )
    out_specs = P(("row", "col"), None)
    return jax.shard_map(body, mesh=mesh, in_specs=in_specs, out_specs=out_specs, check_vma=False)
```

```python
import jax
import jax.numpy as jnp
from jax import lax
from jax.experimental import pallas as pl
from jax.experimental.pallas import tpu as pltpu
from jax.sharding import PartitionSpec as P

LANES = 128
SUBLANES = 8
FETCHES = 1
SMALL = pltpu.CompilerParams(vmem_limit_bytes=8 << 20)
SUMS = pltpu.CompilerParams(vmem_limit_bytes=8 << 20)


def general(messages, dst_local, counts, degrees):
    slots = messages.shape[3]
    width = messages.shape[4]
    owned = degrees.shape[0]
    slot_index = lax.broadcasted_iota(jnp.int32, counts.shape + (slots,), 3)
    alive_mask = (slot_index < counts[..., None]).astype(jnp.float32)
    masked = messages * alive_mask[..., None]

    def exchange(x):
        x = lax.all_to_all(x, "row", split_axis=1, concat_axis=0, tiled=True)
        return lax.all_to_all(x, "col", split_axis=2, concat_axis=1, tiled=True)

    received, labels = exchange(masked), exchange(dst_local)
    summed = jax.ops.segment_sum(received.reshape(-1, width), labels.reshape(-1), num_segments=owned)
    scale = jnp.maximum(degrees, 1).astype(jnp.float32)
    return summed / scale[:, None]


def in_hbm(x):
    return pltpu.with_memory_space_constraint(x, pltpu.HBM)


TUNED = {
    16: (
        (11, 8, 5, 3, 9, 10, 4, 2, 15, 12, 7, 14, 6, 1, 13, 0),
        (11, 2, 5, 3, 4, 6, 9, 8, 15, 12, 7, 14, 10, 1, 13, 0),
    ),
}


def exchange_plan(rows):
    first = rows * 3 // 4 - 1
    order = (first, *(r for r in range(1, rows) if r != first), 0)
    return TUNED.get(rows, (order, order)), range(rows // 2, rows)


def pick(index, values):
    return sum(jnp.where(index == i, v, 0) for i, v in enumerate(values) if v)


def pack_kernel(orders, swapped, *refs):
    counts_hbm, dst_hbm, degrees_hbm, messages_hbm, out_ref, share_ref = refs[:6]
    counts_ref, dst_ref, degrees_ref, messages_ref, sems = refs[6:]
    groups, _, slots, width = messages_ref.shape
    owned = degrees_ref.shape[1]
    small = 3
    pieces = sems.shape[0] - small
    size = groups // pieces
    sides = [(counts_hbm, counts_ref), (dst_hbm, dst_ref), (degrees_hbm, degrees_ref)]
    for i in range(pieces):
        piece = pl.ds(i * size, size)
        sides.append((messages_hbm.at[piece], messages_ref.at[piece]))
    fetches = [pltpu.make_async_copy(*side, sems.at[i]) for i, side in enumerate(sides)]
    for fetch in fetches:
        fetch.start()
    half = slots // 2
    live = slots + half
    pitch = live + 1
    row = lax.axis_index("row")
    second_group = lax.axis_index("col") ^ pick(row, [int(r in swapped) for r in range(groups)])
    places = [jnp.where(second_group == 1, orders[1].index(g), orders[0].index(g)) for g in range(groups)]
    place = pick(row, [orders[0].index(r) for r in range(groups)])
    place = jnp.where(second_group == 1, pick(row, [orders[1].index(r) for r in range(groups)]), place)
    lane = lax.broadcasted_iota(jnp.int32, (groups, width), 1)
    group = lax.broadcasted_iota(jnp.int32, (groups, width), 0)
    fill = jnp.zeros((groups, width - slots), jnp.int32)
    for fetch in fetches[:small]:
        fetch.wait()
    full = [counts_ref[0, g] == slots for g in range(groups)]
    full_rows = jnp.zeros((groups, width), jnp.int32)
    for g in range(groups):
        full_rows = jnp.where(group == g, full[g].astype(jnp.int32), full_rows)
    first = jnp.concatenate([dst_ref[pl.ds(0, groups, stride=2), :], fill], axis=1)
    second = jnp.concatenate([dst_ref[pl.ds(1, groups, stride=2), :], fill], axis=1) + owned
    by_half = pltpu.roll(second, half, 1)
    by_full = pltpu.roll(second, slots, 1)
    when_full = jnp.where(lane < slots, first, by_full)
    when_half = jnp.where(lane < half, first, by_half)
    labels = jnp.where(lane < live, jnp.where(full_rows == 1, when_full, when_half), 0)
    labels = pltpu.roll(labels.astype(jnp.float32), lax.rem(place * slots, width), 1)
    for g in range(groups):
        out_ref[pl.ds(places[g] * pitch + live, 1), :] = labels[g : g + 1, :]
    for start in range(0, owned, width):
        scale = jnp.maximum(degrees_ref[0:1, start : start + width], 1).astype(jnp.float32)
        share_ref[start : start + width, :] = jnp.transpose(jnp.broadcast_to(1.0 / scale, (width, width)))
    for g in range(groups):
        if g % size == 0:
            fetches[small + g // size].wait()
        base = places[g] * pitch
        a0 = messages_ref[g, 0, :half, :]
        a1 = messages_ref[g, 0, half:, :]
        b0 = messages_ref[g, 1, :half, :]
        b1 = messages_ref[g, 1, half:, :]
        out_ref[pl.ds(base, half), :] = a0
        out_ref[pl.ds(base + half, half), :] = jnp.where(full[g], a1, b0)
        out_ref[pl.ds(base + slots, half), :] = jnp.where(full[g], b0, b1)


def slot_values(rows, side, received_ref):
    width = received_ref.shape[1]
    pitch = received_ref.shape[0] // rows
    live = pitch - 1
    half = live // 3
    window = 2 * half
    labels = received_ref[pl.ds(live, rows, stride=pitch), :].astype(jnp.int32)
    labels = pltpu.roll(labels, jnp.where(side == 1, width - half, 0), 1)
    place = lax.broadcasted_iota(jnp.int32, (rows, width), 0)
    lane = lax.broadcasted_iota(jnp.int32, (rows, width), 1)
    position = place * window + lax.rem(lane - lax.rem(place * window, width) + width, width)
    inside = position < (place + 1) * window
    parts = []
    for block in range(rows * window // width):
        here = inside & (position >= block * width) & (position < (block + 1) * width)
        parts.append(jnp.sum(jnp.where(here, labels, 0), axis=0, keepdims=True))
    label = jnp.concatenate(parts, axis=1)
    first = side * half
    values = jnp.concatenate([received_ref[pl.ds(p * pitch + first, window), :] for p in range(rows)], axis=0)
    high = values.astype(jnp.bfloat16)
    low = (values - high.astype(jnp.float32)).astype(jnp.bfloat16)
    return jnp.concatenate([high, low], axis=1), label


def range_sums(owned, side, both, label):
    width = both.shape[1] // 2
    vertex = lax.broadcasted_iota(jnp.int32, (owned, both.shape[0]), 0)
    hot = (vertex == label - side * owned).astype(jnp.float32).astype(jnp.bfloat16)
    sums = jnp.dot(hot, both, preferred_element_type=jnp.float32)
    return sums[:, :width] + sums[:, width:]


def side_sums(rows, owned, side, received_ref):
    return range_sums(owned, side, *slot_values(rows, side, received_ref))


def other_kernel(rows, owned, received_ref, other_ref):
    other_ref[...] = side_sums(rows, owned, 1 - lax.axis_index("col"), received_ref)


def own_kernel(rows, owned, received_ref, share_ref, own_ref):
    sums = side_sums(rows, owned, lax.axis_index("col"), received_ref)
    own_ref[...] = sums * share_ref[...]


def paired(rows, messages, dst_local, counts, degrees):
    _, groups, subs, slots, width = messages.shape
    owned = degrees.shape[0]
    pitch = slots + slots // 2 + 1
    orders, swapped = exchange_plan(rows)
    members = [[r * subs + (c ^ int(r in swapped)) for r in order] for c, order in enumerate(orders)]
    total = rows * slots
    vmem = pl.BlockSpec(memory_space=pltpu.VMEM)
    hbm = pl.BlockSpec(memory_space=pltpu.HBM)
    partial = jax.ShapeDtypeStruct((owned, width), jnp.float32)
    packed, share = pl.pallas_call(
        lambda *refs: pack_kernel(orders, swapped, *refs),
        out_shape=[jax.ShapeDtypeStruct((groups * pitch, width), jnp.float32), partial],
        in_specs=[hbm] * 4,
        out_specs=[vmem] * 2,
        scratch_shapes=[
            pltpu.SMEM((subs, groups), jnp.int32),
            pltpu.VMEM((groups * subs, slots), jnp.int32),
            pltpu.VMEM((1, owned), jnp.int32),
            pltpu.VMEM((groups, subs, slots, width), jnp.float32),
            pltpu.SemaphoreType.DMA((3 + FETCHES,)),
        ],
        compiler_params=SMALL,
        name="pack",
    )(
        in_hbm(counts.reshape(groups, subs).T),
        in_hbm(dst_local.reshape(groups * subs, slots)),
        in_hbm(degrees.reshape(1, owned)),
        in_hbm(messages[0]),
    )
    received = lax.all_to_all(
        packed.reshape(groups * pitch, 1, width),
        ("row", "col"),
        split_axis=0,
        concat_axis=0,
        tiled=True,
        axis_index_groups=members,
    ).reshape(groups * pitch, width)
    other = pl.pallas_call(
        lambda *refs: other_kernel(rows, owned, *refs),
        out_shape=partial,
        in_specs=[vmem],
        out_specs=vmem,
        compiler_params=SUMS,
        name="other_sums",
    )(received)
    mine = lax.ppermute(other, "col", [(0, 1), (1, 0)])
    own = pl.pallas_call(
        lambda *refs: own_kernel(rows, owned, *refs),
        out_shape=partial,
        in_specs=[vmem] * 2,
        out_specs=vmem,
        compiler_params=SUMS,
        cost_estimate=pl.CostEstimate(flops=4 * owned * total * width, bytes_accessed=1 << 20, transcendentals=0),
        name="own_sums",
    )(received, share)
    return own + mine * share


def solution(mesh):
    rows, cols = mesh.shape["row"], mesh.shape["col"]

    def body(messages, dst_local, counts, degrees):
        subs, slots, width = messages.shape[2:]
        fits = width == LANES and slots % (2 * SUBLANES) == 0 and rows * slots % width == 0
        if subs == cols == 2 and fits and rows <= 16:
            return paired(rows, messages, dst_local, counts, degrees)
        return general(messages, dst_local, counts, degrees)

    in_specs = (
        P(("row", "col"), None, None, None, None),
        P(("row", "col"), None, None, None),
        P(("row", "col"), None, None),
        P(("row", "col")),
    )
    out_specs = P(("row", "col"), None)
    return jax.shard_map(body, mesh=mesh, in_specs=in_specs, out_specs=out_specs, check_vma=False)
```
